512 devices in a mesh: rows: 32 (over z, x), cols: 16 (over y, core).
Axes of the slice: x: 4, y: 8, z: 8, core: 2. Of those that a mesh axis runs over, the one named last changes fastest.
Arguments:
- row_features: float32 [16384, 64], P('rows'), may hold values from -6 to 6, as said below
- col_features: float32 [65536, 64], P('cols'), may hold values from -6 to 6, as said below
- test_block: bfloat16 [65536, 256], P('cols'), may hold values from -0.0234375 to 0.0234375, as said below
Outputs:
- basis: float32 [16384, 256], P('rows', 'cols')
- projected: float32 [256, 65536], P('rows', 'cols')
The draws below stay inside these ranges and needn't reach their ends.
Inputs may be any that keep to these rules, and one draw needn't show every extreme that they name: `row_features`: independent entries of mean zero and unit variance. `col_features`: independent entries of mean zero and unit variance. `test_block`: independent entries of mean zero and variance 1 / 65536.
All inputs are finite; a program needn't handle non-finite values.
Results may differ from the reference program's by a relative error of at most 0.0095.
Values may be sent and summed in bfloat16 or wider, within the bound.
A program may use at most 64 MiB of HBM per device.

```python
import math
import jax
import jax.numpy as jnp
from jax import lax

F = 64
S = 256
R_DEV = 512
NR = 16384
NC = 65536


def centered(key, shape, spread):
    return spread * jax.random.truncated_normal(key, -6.0, 6.0, shape, jnp.float32)


def draw_row_features(key, part):
    return centered(jax.random.fold_in(key, 11), (NR, F), 1.0)


def draw_col_features(key, part):
    return centered(jax.random.fold_in(key, 23), (NC, F), 1.0)


def draw_test_block(key, part):
    return centered(jax.random.fold_in(key, 37), (NC, S), 1.0 / NC ** 0.5).astype(jnp.bfloat16)


def setup_inputs(seed: int = 0) -> dict:
    splits = jax.random.split(jax.random.key(seed), 4)
    return {
        "row_features": draw_row_features(jax.random.fold_in(splits[3], 71), 0),
        "col_features": draw_col_features(jax.random.fold_in(splits[3], 71), 0),
        "test_block": draw_test_block(jax.random.fold_in(splits[3], 71), 0),
    }


def kernel_tile(rows, cols):
    inner = lax.dot_general(rows.astype(jnp.float32), cols.astype(jnp.float32), (((1,), (1,)), ((), ())), precision=lax.Precision.HIGHEST, preferred_element_type=jnp.float32) * (1.0 / math.sqrt(F))
    shifted = inner + 1.0
    return (shifted * shifted * shifted).astype(jnp.bfloat16)

def reference(row_features, col_features, test_block):
    blocks = row_features.reshape(NR // R_DEV, R_DEV, F)

    def sketch_block(block):
        return jnp.dot(kernel_tile(block, col_features).astype(jnp.float32), test_block.astype(jnp.float32), preferred_element_type=jnp.float32)
    sketch = lax.map(sketch_block, blocks).reshape(NR, S)
    gram = lax.dot_general(sketch.astype(jnp.float32), sketch.astype(jnp.float32), (((0,), (0,)), ((), ())), precision=lax.Precision.HIGHEST, preferred_element_type=jnp.float32)
    lower = jnp.linalg.cholesky(gram)
    basis = jax.scipy.linalg.solve_triangular(lower, sketch.T, lower=True).T
    basis_b = basis.astype(jnp.bfloat16).reshape(NR // R_DEV, R_DEV, S)

    def accumulate(total, pair):
        block, qblock = pair
        tile = kernel_tile(block, col_features)
        part = lax.dot_general(qblock.astype(jnp.float32), tile.astype(jnp.float32), (((0,), (0,)), ((), ())), preferred_element_type=jnp.float32)
        part = lax.optimization_barrier(part.astype(jnp.bfloat16))
        return (total + part.astype(jnp.float32), None)
    projected, _ = lax.scan(accumulate, jnp.zeros((S, NC), jnp.float32), (blocks, basis_b))
    return (basis, projected)
```

```python
import functools
import math

import jax
import jax.numpy as jnp
from jax import lax
from jax.experimental import pallas as pl
from jax.experimental.pallas import tpu as pltpu
from jax.sharding import PartitionSpec as P

MESH = pl.DeviceIdType.MESH
F32, BF16 = jnp.float32, jnp.bfloat16
ALONG_X = 4
PANEL = 16
CHUNK = 512


def far_first(length):
    return sorted(range(1, length), key=lambda i: -min(i, length - i))


def split2(v):
    high = v.astype(BF16)
    return high, (v - high.astype(F32)).astype(BF16)


def split3(v):
    high = v.astype(BF16)
    rest = v - high.astype(F32)
    mid = rest.astype(BF16)
    return high, mid, (rest - mid.astype(F32)).astype(BF16)


def dot(a, b, dims=((1,), (0,))):
    return lax.dot_general(a, b, (dims, ((), ())), preferred_element_type=F32)


def cubed(inner):
    shifted = inner + 1.0
    return (shifted * shifted * shifted).astype(BF16)


def left_terms(features_t, scale):
    high, low = split2(features_t * scale)
    return jnp.concatenate([high, high, low], axis=0).T


def right_terms(features_t, scale):
    high, low = split2(features_t * scale)
    return jnp.concatenate([high, low, high], axis=0)


def eliminate(work):
    n = work.shape[0]
    row = lax.broadcasted_iota(jnp.int32, (PANEL, 1), 0)
    for p in range(n // PANEL):
        first = p * PANEL
        base = (first // 128) * 128
        offset = first - base
        end = n + ((first + PANEL + 127) // 128) * 128
        panel = work[first : first + PANEL, base:end]
        tiles = panel.shape[1] // 128
        column = [
            jnp.broadcast_to(panel[:, offset + j : offset + j + 1], (PANEL, 128))
            for j in range(PANEL)
        ]
        for k in range(PANEL):
            inverse_root = lax.rsqrt(column[k][k : k + 1, :])
            lower = column[k] * inverse_root
            for j in range(k + 1, PANEL):
                column[j] = column[j] - lower * lower[j : j + 1, :]
            pivot_row = panel[k : k + 1, :] * jnp.concatenate([inverse_root] * tiles, axis=1)
            below = jnp.concatenate([jnp.where(row > k, lower, 0.0)] * tiles, axis=1)
            panel = jnp.where(
                row == k, jnp.broadcast_to(pivot_row, panel.shape), panel - below * pivot_row
            )
        work[first : first + PANEL, base:end] = panel
        after = first + PANEL
        if after < n:
            high, mid, low = split3(panel)
            start = (after // 128) * 128
            keep = slice(start - base, n - base)
            left = jnp.concatenate([t[:, keep] for t in (high, high, mid, high, mid, low)], axis=0)
            right = jnp.concatenate([high, mid, high, low, mid, high], axis=0)
            work[after:, base:end] = work[after:, base:end] - dot(left.T[after - start :, :], right)


def kernel(
    nx, nz, nc,
    row_ref, col_ref, test_ref, basis_ref, out_ref,
    row_left, col_left, partial, rs_send, rs_recv, rows_recv, own_sketch, sketch,
    tile_t, gram, gx_recv, gz_send, gz_recv, gy_send, gram_all,
    p_send, p_recv, work, o_send, o_recv,
    rows_sem, rs_sem, ag_sem, gx_sem, xag_sem, fwd_sem, gz_sem, gy_sem, p_sem, o_sem,
):
    r, c = lax.axis_index("rows"), lax.axis_index("cols")
    z, x = r // nx, lax.rem(r, nx)
    rows, size = partial.shape
    width = row_ref.shape[0]
    scale = 1.0 / math.sqrt(width)
    columns = col_ref.shape[1]
    per_x = columns // nx
    per_z = per_x // nz
    half = lax.rem(c, 2)

    def at_x(i):
        return (z * nx + lax.rem(x + i, nx), c)

    def at_z(i):
        return (lax.rem(z + i, nz) * nx + x, c)

    def at_c(i):
        return (r, lax.rem(c + i, nc))

    def at_zx(i, j):
        return (lax.rem(z + i, nz) * nx + lax.rem(x + j, nx), c)

    around = [(i, j) for i in range(nz) for j in range(nx) if (i, j) != (0, 0)]
    around.sort(key=lambda ij: -min(ij[0], nz - ij[0]) - min(ij[1], nx - ij[1]))

    def copy(src, dst, sems, k, device):
        return pltpu.make_async_remote_copy(
            src_ref=src,
            dst_ref=dst,
            send_sem=sems.at[0, k],
            recv_sem=sems.at[1, k],
            device_id=device,
            device_id_type=MESH,
        )

    barrier = pltpu.get_barrier_semaphore()
    for i in range(1, nc):
        pl.semaphore_signal(barrier, inc=1, device_id=at_c(i), device_id_type=MESH)
    for i, j in around:
        pl.semaphore_signal(barrier, inc=1, device_id=at_zx(i, j), device_id_type=MESH)

    row_left[...] = left_terms(row_ref[...], scale)
    partial[...] = jnp.zeros_like(partial)

    @pl.loop(0, columns // CHUNK)
    def _(n):
        at = pl.ds(pl.multiple_of(n * CHUNK, CHUNK), CHUNK)
        tile = cubed(dot(row_left[...], right_terms(col_ref[:, at], 1.0)))
        partial[...] += dot(tile, test_ref[at, :])

    rs_send[...] = partial[...].astype(BF16).reshape(rs_send.shape)

    pl.semaphore_wait(barrier, nc - 1 + len(around))

    piece = rows // nc
    rs = {i: copy(rs_send.at[lax.rem(c + i, nc)], rs_recv.at[i - 1], rs_sem, i - 1, at_c(i)) for i in far_first(nc)}
    for i in far_first(nc):
        rs[i].start()
    feat = [copy(row_ref, rows_recv.at[i - 1], rows_sem, i - 1, at_x(i)) for i in range(1, nx)]
    for one in feat:
        one.start()
    own = pl.ds(pl.multiple_of(x * per_x, per_x), per_x)
    col_left[...] = left_terms(col_ref[:, own], 1.0)
    total = partial[pl.ds(pl.multiple_of(c * piece, piece), piece), :]
    for i in range(1, nc):
        rs[i].wait_recv()
        total = total + rs_recv[i - 1].astype(F32)
    own_sketch[...] = total.astype(BF16)
    sketch[x, c] = own_sketch[...]

    ag = {i: copy(own_sketch, sketch.at[x, c], ag_sem, i - 1, at_c(i)) for i in far_first(nc)}
    for i in far_first(nc):
        ag[i].start()

    block = min(256, per_x)
    for i in range(nx):
        if i:
            feat[i - 1].wait_recv()
        source = rows_recv[i - 1] if i else row_ref[...]
        right = right_terms(source, scale)
        at_block = lax.rem(x + nx - i, nx)

        @pl.loop(0, per_x // block)
        def _(m):
            at = pl.ds(pl.multiple_of(m * block, block), block)
            tile_t[at_block, at, :] = cubed(dot(col_left[at, :], right))

    for i in range(1, nc):
        ag[i].wait_recv()

    held = sketch[x].reshape(rows, size)
    gram[...] = dot(held, held, ((0,), (0,))).reshape(gram.shape)
    gx = [copy(gram.at[c], gx_recv.at[i - 1], gx_sem, i - 1, at_x(i)) for i in range(1, nx)]
    for one in gx:
        one.start()
    mine = pl.ds(half * (nc // 2), nc // 2)
    xag = [
        copy(sketch.at[x, mine], sketch.at[x, mine], xag_sem, i - 1, at_x(i)) for i in range(1, nx)
    ]
    for one in xag:
        one.start()
    slice_sum = gram[c]
    for i in range(1, nx):
        gx[i - 1].wait_recv()
        slice_sum = slice_sum + gx_recv[i - 1]
    gz_send[...] = slice_sum
    gz = {i: copy(gz_send, gz_recv.at[i - 1], gz_sem, i - 1, at_z(i)) for i in far_first(nz)}
    for i in far_first(nz):
        gz[i].start()

    sibling = (r, c + 1 - 2 * half)
    fwd = []
    for i in range(1, nx):
        xag[i - 1].wait_recv()
        there = sketch.at[lax.rem(x + nx - i, nx), mine]
        fwd.append(copy(there, there, fwd_sem, i - 1, sibling))
        fwd[-1].start()

    for i in range(1, nz):
        gz[i].wait_recv()
        slice_sum = slice_sum + gz_recv[i - 1]
    gy_send[...] = slice_sum
    gram_all[c] = slice_sum
    gy = {i: copy(gy_send, gram_all.at[c], gy_sem, i - 1, at_c(i)) for i in far_first(nc)}
    for i in far_first(nc):
        gy[i].start()

    for i in range(1, nx):
        fwd[i - 1].wait_recv()
    block = min(2 * per_z, per_x)

    @pl.loop(0, per_x // block)
    def _(m):
        at = pl.ds(pl.multiple_of(m * block, block), block)
        total = dot(tile_t[0, at, :], sketch[0].reshape(rows, size))
        for i in range(1, nx):
            total = total + dot(tile_t[i, at, :], sketch[i].reshape(rows, size))
        count = block // per_z
        p_send[pl.ds(m * count, count)] = total.astype(BF16).reshape(count, per_z, size)

    ps = {i: copy(p_send.at[lax.rem(z + i, nz)], p_recv.at[i - 1], p_sem, i - 1, at_z(i)) for i in far_first(nz)}
    for i in far_first(nz):
        ps[i].start()

    for i in range(1, nc):
        gy[i].wait_recv()
    work[:, :size] = gram_all[...].reshape(size, size)
    diagonal = lax.broadcasted_iota(jnp.int32, (size, size), 0)
    work[:, size:] = jnp.where(diagonal == lax.broadcasted_iota(jnp.int32, (size, size), 1), 1.0, 0.0)
    eliminate(work)

    product = p_send[z].astype(F32)
    for i in range(1, nz):
        ps[i].wait_recv()
        product = product + p_recv[i - 1].astype(F32)
    inverse_high, inverse_low = split2(work[:, size:])
    product_high, product_low = split2(product)
    result = dot(
        jnp.concatenate([inverse_high, inverse_high, inverse_low], axis=1),
        jnp.concatenate([product_high, product_low, product_high], axis=1),
        ((1,), (1,)),
    )
    o_send[...] = result.reshape(o_send.shape)
    mine = pl.ds(pl.multiple_of(x * per_x + z * per_z, per_z), per_z)
    outs = []
    for k, (i, j) in enumerate(around):
        target = at_zx(i, j)
        outs.append(copy(o_send.at[target[0]], o_recv.at[:, mine], o_sem, k, target))
        outs[-1].start()
    o_recv[:, mine] = o_send[r]
    share = size // nc
    share_high, share_low = split2(work[pl.ds(pl.multiple_of(c * share, share), share), size:])
    held = sketch[x].reshape(rows, size)
    basis_ref[...] = dot(share_high, held, ((1,), (1,))) + dot(share_low, held, ((1,), (1,)))
    for one in outs:
        one.wait_recv()
    out_ref[...] = o_recv[...]

    for group in (feat, rs.values(), ag.values(), gx, xag, gz.values(), fwd, gy.values(), ps.values(), outs):
        for one in group:
            one.wait_send()


def local(nx, nz, nc, row_features, col_features, test_block):
    rows, width = row_features.shape
    columns, size = test_block.shape
    per_x = columns // nx
    per_z = per_x // nz
    share = size // nc
    piece = rows // nc
    vmem = pltpu.VMEM

    def sems(count):
        return pltpu.SemaphoreType.DMA((2, count))

    basis_t, projected = pl.pallas_call(
        functools.partial(kernel, nx, nz, nc),
        out_shape=(
            jax.ShapeDtypeStruct((share, rows), F32),
            jax.ShapeDtypeStruct((size // (nx * nz), columns), F32),
        ),
        in_specs=[pl.BlockSpec(memory_space=vmem)] * 3,
        out_specs=(pl.BlockSpec(memory_space=vmem),) * 2,
        scratch_shapes=[
            vmem((rows, 3 * width), BF16),
            vmem((per_x, 3 * width), BF16),
            vmem((rows, size), F32),
            vmem((nc, piece, size), BF16),
            vmem((nc - 1, piece, size), BF16),
            vmem((nx - 1, width, rows), F32),
            vmem((piece, size), BF16),
            vmem((nx, nc, piece, size), BF16),
            vmem((nx, per_x, rows), BF16),
            vmem((nc, share, size), F32),
            vmem((nx - 1, share, size), F32),
            vmem((share, size), F32),
            vmem((nz - 1, share, size), F32),
            vmem((share, size), F32),
            vmem((nc, share, size), F32),
            vmem((nz, per_z, size), BF16),
            vmem((nz - 1, per_z, size), BF16),
            vmem((size, 2 * size), F32),
            vmem((nx * nz, size // (nx * nz), per_z), F32),
            vmem((size // (nx * nz), columns), F32),
            sems(nx - 1),
            sems(nc - 1),
            sems(nc - 1),
            sems(nx - 1),
            sems(nx - 1),
            sems(nx - 1),
            sems(nz - 1),
            sems(nc - 1),
            sems(nz - 1),
            sems(nx * nz - 1),
        ],
        compiler_params=pltpu.CompilerParams(
            collective_id=0, has_side_effects=True, vmem_limit_bytes=56 * 1024 * 1024
        ),
    )(row_features.T, col_features.T, test_block)
    return basis_t.T, projected


def solution(mesh, nx=ALONG_X):
    nz, nc = mesh.shape["rows"] // nx, mesh.shape["cols"]
    return jax.shard_map(
        functools.partial(local, nx, nz, nc),
        mesh=mesh,
        in_specs=(P("rows", None), P("cols", None), P("cols", None)),
        out_specs=(P("rows", "cols"), P("rows", "cols")),
        check_vma=False,
    )
```

```python
import functools
import math

import jax
import jax.numpy as jnp
from jax import lax
from jax.experimental import pallas as pl
from jax.experimental.pallas import tpu as pltpu
from jax.sharding import PartitionSpec as P

MESH = pl.DeviceIdType.MESH
F32, BF16 = jnp.float32, jnp.bfloat16
ALONG_X = 4
PANEL = 16
STEPS = 2
VMEM_LIMIT = 56_300_000


def far_first(length):
    return sorted(range(1, length), key=lambda i: -min(i, length - i))


def split2(v):
    high = v.astype(BF16)
    return high, (v - high.astype(F32)).astype(BF16)


def split3(v):
    high = v.astype(BF16)
    rest = v - high.astype(F32)
    mid = rest.astype(BF16)
    return high, mid, (rest - mid.astype(F32)).astype(BF16)


def dot(a, b, dims=((1,), (0,))):
    return lax.dot_general(a, b, (dims, ((), ())), preferred_element_type=F32)


def cubed(inner):
    shifted = inner + 1.0
    return (shifted * shifted * shifted).astype(BF16)


def left_terms(features_t, scale):
    high, low = split2(features_t * scale)
    return jnp.concatenate([high, high, low], axis=0).T


def right_terms(features_t, scale):
    high, low = split2(features_t * scale)
    return jnp.concatenate([high, low, high], axis=0)


def eliminate(work):
    n = work.shape[0]
    row = lax.broadcasted_iota(jnp.int32, (PANEL, 1), 0)
    for p in range(n // PANEL):
        first = p * PANEL
        base = (first // 128) * 128
        offset = first - base
        end = n + ((first + PANEL + 127) // 128) * 128
        panel = work[first : first + PANEL, base:end]
        tiles = panel.shape[1] // 128
        column = [
            jnp.broadcast_to(panel[:, offset + j : offset + j + 1], (PANEL, 128))
            for j in range(PANEL)
        ]
        for k in range(PANEL):
            inverse_root = lax.rsqrt(column[k][k : k + 1, :])
            lower = column[k] * inverse_root
            for j in range(k + 1, PANEL):
                column[j] = column[j] - lower * lower[j : j + 1, :]
            pivot_row = panel[k : k + 1, :] * jnp.concatenate([inverse_root] * tiles, axis=1)
            below = jnp.concatenate([jnp.where(row > k, lower, 0.0)] * tiles, axis=1)
            panel = jnp.where(
                row == k, jnp.broadcast_to(pivot_row, panel.shape), panel - below * pivot_row
            )
        work[first : first + PANEL, base:end] = panel
        after = first + PANEL
        if after < n:
            high, mid, low = split3(panel)
            start = (after // 128) * 128
            keep = slice(start - base, n - base)
            left = jnp.concatenate([t[:, keep] for t in (high, high, mid, high, mid, low)], axis=0)
            right = jnp.concatenate([high, mid, high, low, mid, high], axis=0)
            work[after:, base:end] = work[after:, base:end] - dot(left.T[after - start :, :], right)


def kernel(
    nx, nz, nc,
    row_hbm, col_hbm, test_hbm, basis_ref, out_ref,
    row_ref, col_ref, test_ref,
    row_left, col_left, partial, pair_send, pair_recv, rs_send, rs_recv, rows_recv, own_sketch, sketch,
    tile_t, gram, gx_recv, gz_send, gz_recv, gy_send, gram_all,
    p_send, p_recv, work, o_send, o_recv,
    in_sem, sent_sem, rows_sem, pair_sem, rs_sem, ag_sem, ag2_sem, gx_sem, xag_sem, fwd_sem, gz_sem, gy_sem, gy2_sem,
    p_sem, o_sem,
):
    r, c = lax.axis_index("rows"), lax.axis_index("cols")
    z, x = r // nx, lax.rem(r, nx)
    ny = nc // 2
    y, half = c // 2, lax.rem(c, 2)
    rows, size = partial.shape
    piece = rows // nc
    width = row_ref.shape[0]
    scale = 1.0 / math.sqrt(width)
    columns = col_ref.shape[1]
    per_x = columns // nx
    per_z = per_x // nz
    place = half * ny + y

    def at_x(i):
        return (z * nx + lax.rem(x + i, nx), c)

    def at_z(i):
        return (lax.rem(z + i, nz) * nx + x, c)

    def at_y(i):
        return (r, lax.rem(y + i, ny) * 2 + half)

    def at_zx(i, j):
        return (lax.rem(z + i, nz) * nx + lax.rem(x + j, nx), c)

    sibling = (r, c + 1 - 2 * half)
    around = [(i, j) for i in range(nz) for j in range(nx) if (i, j) != (0, 0)]
    around.sort(key=lambda ij: -min(ij[0], nz - ij[0]) - min(ij[1], nx - ij[1]))

    def copy(group, src, dst, recv_sem, device):
        return pltpu.make_async_remote_copy(
            src_ref=src,
            dst_ref=dst,
            send_sem=sent_sem.at[group],
            recv_sem=recv_sem,
            device_id=device,
            device_id_type=MESH,
        )

    def wait_sent(group, whole):
        copy(group, whole, whole, in_sem.at[0], sibling).wait_send()

    steps = [slice(n, n + columns // STEPS) for n in range(0, columns, columns // STEPS)]
    pieces = [(row_hbm, row_ref)]
    for at in steps:
        pieces += [(col_hbm.at[:, at], col_ref.at[:, at]), (test_hbm.at[at, :], test_ref.at[at, :])]
    loads = [pltpu.make_async_copy(src, dst, in_sem.at[k]) for k, (src, dst) in enumerate(pieces)]
    for one in loads:
        one.start()
    barrier = pltpu.get_barrier_semaphore()
    pl.semaphore_signal(barrier, inc=1, device_id=sibling, device_id_type=MESH)
    for i in far_first(ny):
        pl.semaphore_signal(barrier, inc=1, device_id=at_y(i), device_id_type=MESH)
    for i, j in around:
        pl.semaphore_signal(barrier, inc=1, device_id=at_zx(i, j), device_id_type=MESH)

    loads[0].wait()
    row_left[...] = left_terms(row_ref[...], scale)
    for n, at in enumerate(steps):
        loads[2 * n + 1].wait()
        tile = cubed(dot(row_left[...], right_terms(col_ref[:, at], 1.0)))
        loads[2 * n + 2].wait()
        share = dot(tile, test_ref[at, :])
        partial[...] = partial[...] + share if n else share

    def half_of(which):
        return pl.ds(pl.multiple_of(which * (rows // 2), rows // 2), rows // 2)

    pair_send[...] = partial[half_of(1 - half), :].astype(BF16)
    pl.semaphore_wait(barrier, ny + len(around))

    pair = copy(0, pair_send, pair_recv, pair_sem.at[0], sibling)
    pair.start()
    feat = [copy(1, row_ref, rows_recv.at[i - 1], rows_sem.at[i - 1], at_x(i)) for i in range(1, nx)]
    for one in feat:
        one.start()
    pair.wait_recv()
    partial[half_of(half), :] += pair_recv[...].astype(F32)
    rs_send[...] = partial[half_of(half), :].astype(BF16).reshape(rs_send.shape)
    rs = [copy(2, rs_send.at[lax.rem(y + i, ny)], rs_recv.at[i - 1], rs_sem.at[0], at_y(i)) for i in far_first(ny)]
    for one in rs:
        one.start()
    own = pl.ds(pl.multiple_of(x * per_x, per_x), per_x)
    col_left[...] = left_terms(col_ref[:, own], 1.0)
    total = partial[pl.ds(pl.multiple_of(place * piece, piece), piece), :]
    copy(2, rs_recv, rs_recv, rs_sem.at[0], sibling).wait_recv()
    for i in range(1, ny):
        total = total + rs_recv[i - 1].astype(F32)
    own_sketch[...] = total.astype(BF16)
    sketch[x, place] = own_sketch[...]

    ag = {i: copy(3, own_sketch, sketch.at[x, place], ag_sem.at[i - 1], at_y(i)) for i in far_first(ny)}
    for i in far_first(ny):
        ag[i].start()
    copy(4, own_sketch, sketch.at[x, place], ag2_sem.at[0], sibling).start()

    block = min(256, per_x)
    for i in range(nx):
        if i:
            feat[i - 1].wait_recv()
        source = rows_recv[i - 1] if i else row_ref[...]
        right = right_terms(source, scale)
        at_block = lax.rem(x + nx - i, nx)

        @pl.loop(0, per_x // block)
        def _(m):
            at = pl.ds(pl.multiple_of(m * block, block), block)
            tile_t[at_block, at, :] = cubed(dot(col_left[at, :], right))

    near_first = far_first(ny)[::-1]
    for i in near_first:
        ag[i].wait_recv()
        there = sketch.at[x, half * ny + lax.rem(y + ny - i, ny)]
        copy(4, there, there, ag2_sem.at[0], sibling).start()
    mine = pl.ds(half * ny, ny)
    other = pl.ds((1 - half) * ny, ny)
    copy(4, sketch.at[x, other], sketch.at[x, other], ag2_sem.at[0], sibling).wait_recv()

    held = sketch[x].reshape(rows, size)
    whole = dot(held, held, ((0,), (0,)))
    top = size // 2
    part = top // nc
    gram[:, 0] = whole[:top, :top].reshape(nc, part, top)
    gram[:, 1] = whole[:top, top:].reshape(nc, part, top)
    gram[:, 2] = whole[top:, top:].reshape(nc, part, top)
    gx = [copy(5, gram.at[place], gx_recv.at[i - 1], gx_sem.at[0], at_x(i)) for i in range(1, nx)]
    for one in gx:
        one.start()
    xag = [copy(6, sketch.at[x, mine], sketch.at[x, mine], xag_sem.at[i - 1], at_x(i)) for i in range(1, nx)]
    for one in xag:
        one.start()
    slice_sum = gram[place]
    copy(5, gx_recv, gx_recv, gx_sem.at[0], sibling).wait_recv()
    for i in range(1, nx):
        slice_sum = slice_sum + gx_recv[i - 1]
    gz_send[...] = slice_sum
    gz = [copy(7, gz_send, gz_recv.at[i - 1], gz_sem.at[0], at_z(i)) for i in far_first(nz)]
    for one in gz:
        one.start()

    for i in range(1, nx):
        xag[i - 1].wait_recv()
        there = sketch.at[lax.rem(x + nx - i, nx), mine]
        copy(8, there, there, fwd_sem.at[i - 1], sibling).start()

    copy(7, gz_recv, gz_recv, gz_sem.at[0], sibling).wait_recv()
    for i in range(1, nz):
        slice_sum = slice_sum + gz_recv[i - 1]
    gy_send[...] = slice_sum
    gram_all[place] = slice_sum
    gy = {i: copy(9, gy_send, gram_all.at[place], gy_sem.at[i - 1], at_y(i)) for i in far_first(ny)}
    for i in far_first(ny):
        gy[i].start()
    copy(10, gy_send, gram_all.at[place], gy2_sem.at[0], sibling).start()

    for i in range(1, nx):
        there = sketch.at[lax.rem(x + nx - i, nx), other]
        copy(8, there, there, fwd_sem.at[i - 1], sibling).wait_recv()
    pairs = nz // 2
    for i in far_first(pairs) + [0]:
        to = lax.rem(z // 2 + i, pairs)
        at = pl.ds(pl.multiple_of(to * 2 * per_z, 2 * per_z), 2 * per_z)
        total = dot(tile_t[0, at, :], sketch[0].reshape(rows, size))
        for j in range(1, nx):
            total = total + dot(tile_t[j, at, :], sketch[j].reshape(rows, size))
        p_send[pl.ds(2 * to, 2)] = total.astype(BF16).reshape(2, per_z, size)
        targets = [2 * to, 2 * to + 1] if i else [z + 1 - 2 * lax.rem(z, 2)]
        for t in targets:
            slot = lax.rem(t + nz - z, nz) - 1
            copy(11, p_send.at[t], p_recv.at[slot], p_sem.at[0], (t * nx + x, c)).start()

    for i in near_first:
        gy[i].wait_recv()
        there = gram_all.at[half * ny + lax.rem(y + ny - i, ny)]
        copy(10, there, there, gy2_sem.at[0], sibling).start()
    copy(10, gram_all.at[other], gram_all.at[other], gy2_sem.at[0], sibling).wait_recv()
    work[:top, :top] = gram_all[:, 0].reshape(top, top)
    work[:top, top:size] = gram_all[:, 1].reshape(top, top)
    work[top:, :top] = jnp.zeros((top, top), F32)
    work[top:, top:size] = gram_all[:, 2].reshape(top, top)
    diagonal = lax.broadcasted_iota(jnp.int32, (size, size), 0)
    work[:, size:] = jnp.where(diagonal == lax.broadcasted_iota(jnp.int32, (size, size), 1), 1.0, 0.0)
    eliminate(work)

    product = p_send[z].astype(F32)
    copy(11, p_recv, p_recv, p_sem.at[0], sibling).wait_recv()
    for i in range(1, nz):
        product = product + p_recv[i - 1].astype(F32)
    inverse_high, inverse_low = split2(work[:, size:])
    product_high, product_low = split2(product)
    result = dot(
        jnp.concatenate([inverse_high, inverse_high, inverse_low], axis=1),
        jnp.concatenate([product_high, product_low, product_high], axis=1),
        ((1,), (1,)),
    )
    o_send[...] = result.reshape(o_send.shape)
    spot = pl.ds(pl.multiple_of(x * per_x + z * per_z, per_z), per_z)
    for i, j in around:
        target = at_zx(i, j)
        copy(12, o_send.at[target[0]], o_recv.at[:, spot], o_sem.at[0], target).start()
    o_recv[:, spot] = o_send[r]
    share = size // nc
    take = pl.ds(pl.multiple_of(c * share, share), share)
    share_high, share_low = split2(work[take, size:])
    held = sketch[x].reshape(rows, size)
    basis_ref[...] = dot(share_high, held, ((1,), (1,))) + dot(share_low, held, ((1,), (1,)))
    wait_sent(0, pair_send)
    wait_sent(1, rows_recv)
    wait_sent(2, rs_recv)
    wait_sent(3, rs_recv)
    wait_sent(4, rs_send)
    wait_sent(5, gx_recv)
    wait_sent(6, sketch.at[pl.ds(0, nx - 1), mine])
    wait_sent(7, gz_recv)
    wait_sent(8, sketch.at[pl.ds(0, nx - 1), mine])
    wait_sent(9, gram_all.at[pl.ds(0, ny - 1)])
    wait_sent(10, gram_all.at[mine])
    wait_sent(11, p_recv)
    others = o_send.at[pl.ds(0, len(around))]
    copy(12, others, others, o_sem.at[0], sibling).wait()
    out_ref[...] = o_recv[...]


def local(nx, nz, nc, row_features, col_features, test_block):
    rows, width = row_features.shape
    columns, size = test_block.shape
    per_x = columns // nx
    per_z = per_x // nz
    share = size // nc
    piece = rows // nc
    vmem = pltpu.VMEM

    def sems(count):
        return pltpu.SemaphoreType.DMA((count,))

    basis_t, projected = pl.pallas_call(
        functools.partial(kernel, nx, nz, nc),
        out_shape=(
            jax.ShapeDtypeStruct((share, rows), F32),
            jax.ShapeDtypeStruct((size // (nx * nz), columns), F32),
        ),
        in_specs=[pl.BlockSpec(memory_space=pl.ANY)] * 3,
        out_specs=(pl.BlockSpec(memory_space=vmem),) * 2,
        scratch_shapes=[
            vmem((width, rows), F32),
            vmem((width, columns), F32),
            vmem((columns, size), BF16),
            vmem((rows, 3 * width), BF16),
            vmem((per_x, 3 * width), BF16),
            vmem((rows, size), F32),
            vmem((rows // 2, size), BF16),
            vmem((rows // 2, size), BF16),
            vmem((nc // 2, piece, size), BF16),
            vmem((nc // 2 - 1, piece, size), BF16),
            vmem((nx - 1, width, rows), F32),
            vmem((piece, size), BF16),
            vmem((nx, nc, piece, size), BF16),
            vmem((nx, per_x, rows), BF16),
            vmem((nc, 3, size // 2 // nc, size // 2), F32),
            vmem((nx - 1, 3, size // 2 // nc, size // 2), F32),
            vmem((3, size // 2 // nc, size // 2), F32),
            vmem((nz - 1, 3, size // 2 // nc, size // 2), F32),
            vmem((3, size // 2 // nc, size // 2), F32),
            vmem((nc, 3, size // 2 // nc, size // 2), F32),
            vmem((nz, per_z, size), BF16),
            vmem((nz - 1, per_z, size), BF16),
            vmem((size, 2 * size), F32),
            vmem((nx * nz, size // (nx * nz), per_z), F32),
            vmem((size // (nx * nz), columns), F32),
            sems(1 + 2 * STEPS),
            sems(13),
            sems(nx - 1),
            sems(1),
            sems(1),
            sems(nc // 2 - 1),
            sems(1),
            sems(1),
            sems(nx - 1),
            sems(nx - 1),
            sems(1),
            sems(nc // 2 - 1),
            sems(1),
            sems(1),
            sems(1),
        ],
        compiler_params=pltpu.CompilerParams(
            collective_id=0, has_side_effects=True, vmem_limit_bytes=VMEM_LIMIT
        ),
    )(row_features.T, col_features.T, test_block)
    return basis_t.T, projected


def solution(mesh, nx=ALONG_X):
    nz, nc = mesh.shape["rows"] // nx, mesh.shape["cols"]
    return jax.shard_map(
        functools.partial(local, nx, nz, nc),
        mesh=mesh,
        in_specs=(P("rows", None), P("cols", None), P("cols", None)),
        out_specs=(P("rows", "cols"), P("rows", "cols")),
        check_vma=False,
    )
```

```python
import functools
import math

import jax
import jax.numpy as jnp
from jax import lax
from jax.experimental import pallas as pl
from jax.experimental.pallas import tpu as pltpu
from jax.sharding import PartitionSpec as P

MESH = pl.DeviceIdType.MESH
F32, BF16 = jnp.float32, jnp.bfloat16
ALONG_X = 4
PANEL = 32
PART = 16
STEPS = 2
VMEM_LIMIT = 56_300_000


def far_first(length):
    return sorted(range(1, length), key=lambda i: -min(i, length - i))


def split2(v):
    high = v.astype(BF16)
    return high, (v - high.astype(F32)).astype(BF16)


def split3(v):
    high = v.astype(BF16)
    rest = v - high.astype(F32)
    mid = rest.astype(BF16)
    return high, mid, (rest - mid.astype(F32)).astype(BF16)


def dot(a, b, dims=((1,), (0,))):
    return lax.dot_general(a, b, (dims, ((), ())), preferred_element_type=F32)


def cubed(inner):
    shifted = inner + 1.0
    return (shifted * shifted * shifted).astype(BF16)


def left_terms(features_t, scale):
    high, low = split2(features_t * scale)
    return jnp.concatenate([high, high, low], axis=0).T


def right_terms(features_t, scale):
    high, low = split2(features_t * scale)
    return jnp.concatenate([high, low, high], axis=0)


def eliminate(work):
    n = work.shape[0]
    row = lax.broadcasted_iota(jnp.int32, (8, 128), 0)
    groups = PANEL // 8
    for first in range(0, n, PANEL):
        after = first + PANEL
        base = (first // 128) * 128
        offset = first - base
        end = n + ((after + 127) // 128) * 128
        tiles = range(base, end, 128)
        panel = [
            [work[first + 8 * g : first + 8 * g + 8, t : t + 128] for t in tiles] for g in range(groups)
        ]
        for part in range(0, PANEL, PART):
            column = {
                j: {
                    g: jnp.broadcast_to(panel[g][0][:, offset + j : offset + j + 1], (8, 128))
                    for g in range(j // 8, groups)
                }
                for j in range(part, part + PART)
            }
            for k in range(part, part + PART):
                own, at = k // 8, k % 8
                inverse_root = lax.rsqrt(column[k][own][at : at + 1, :])
                lower = {g: v * inverse_root for g, v in column[k].items()}
                for j in range(k + 1, part + PART):
                    factor = lower[j // 8][j % 8 : j % 8 + 1, :]
                    column[j] = {g: v - lower[g] * factor for g, v in column[j].items()}
                below = jnp.where(row > at, lower[own], 0.0)
                for t in range(len(tiles)):
                    pivot_row = panel[own][t][at : at + 1, :] * inverse_root
                    panel[own][t] = jnp.where(
                        row == at,
                        jnp.broadcast_to(pivot_row, (8, 128)),
                        panel[own][t] - below * pivot_row,
                    )
                    for g in range(own + 1, groups):
                        panel[g][t] = panel[g][t] - lower[g] * pivot_row
        panel = jnp.concatenate([jnp.concatenate(g, axis=1) for g in panel], axis=0)
        work[first:after, base:end] = panel
        if after < n:
            high, mid, low = split3(panel)
            start = (after // 128) * 128
            keep = slice(start - base, n - base)
            left = jnp.concatenate([t[:, keep] for t in (high, high, mid, high, mid, low)], axis=0)
            right = jnp.concatenate([high, mid, high, low, mid, high], axis=0)
            work[after:, base:end] = work[after:, base:end] - dot(left.T[after - start :, :], right)


def kernel(
    nx, nz, nc,
    row_hbm, col_hbm, test_hbm, basis_ref, out_ref,
    row_ref, col_ref, test_ref,
    row_left, col_left, partial, pair_send, pair_recv, rs_send, rs_recv, rows_recv, own_sketch, sketch,
    tile_t, gram, gx_recv, gz_send, gz_recv, gy_send, gram_all,
    p_send, p_recv, work, o_send, o_recv,
    in_sem, sent_sem, far_sem, rows_sem, pair_sem, rs_sem, ag_sem, ag2_sem, gx_sem, xag_sem, fwd_sem, gz_sem, gy_sem, gy2_sem,
    p_sem, o_sem,
):
    r, c = lax.axis_index("rows"), lax.axis_index("cols")
    z, x = r // nx, lax.rem(r, nx)
    ny = nc // 2
    y, half = c // 2, lax.rem(c, 2)
    rows, size = 2 * partial.shape[0], partial.shape[1]
    piece = rows // nc
    width = row_ref.shape[0]
    scale = 1.0 / math.sqrt(width)
    columns = col_ref.shape[1]
    per_x = columns // nx
    per_z = per_x // nz
    place = half * ny + y

    def at_x(i):
        return (z * nx + lax.rem(x + i, nx), c)

    def at_z(i):
        return (lax.rem(z + i, nz) * nx + x, c)

    def at_y(i):
        return (r, lax.rem(y + i, ny) * 2 + half)

    def at_zx(i, j):
        return (lax.rem(z + i, nz) * nx + lax.rem(x + j, nx), c)

    sibling = (r, c + 1 - 2 * half)
    around = [(i, j) for i in range(nz) for j in range(nx) if (i, j) != (0, 0)]
    around.sort(key=lambda ij: -min(ij[0], nz - ij[0]) - min(ij[1], nx - ij[1]))

    def copy(group, src, dst, recv_sem, device):
        return pltpu.make_async_remote_copy(
            src_ref=src,
            dst_ref=dst,
            send_sem=sent_sem.at[group],
            recv_sem=recv_sem,
            device_id=device,
            device_id_type=MESH,
        )

    def wait_sent(group, whole):
        copy(group, whole, whole, in_sem.at[0], sibling).wait_send()

    steps = [slice(n, n + columns // STEPS) for n in range(0, columns, columns // STEPS)]
    pieces = [(row_hbm, row_ref)]
    for at in steps:
        pieces += [(col_hbm.at[:, at], col_ref.at[:, at]), (test_hbm.at[at, :], test_ref.at[at, :])]
    loads = [pltpu.make_async_copy(src, dst, in_sem.at[k]) for k, (src, dst) in enumerate(pieces)]
    for one in loads:
        one.start()
    barrier = pltpu.get_barrier_semaphore()
    pl.semaphore_signal(barrier, inc=1, device_id=sibling, device_id_type=MESH)
    for i in far_first(ny):
        pl.semaphore_signal(barrier, inc=1, device_id=at_y(i), device_id_type=MESH)
    for i, j in around:
        pl.semaphore_signal(barrier, inc=1, device_id=at_zx(i, j), device_id_type=MESH)

    loads[0].wait()
    row_left[...] = left_terms(row_ref[...], scale)
    def half_of(which):
        return pl.ds(pl.multiple_of(which * (rows // 2), rows // 2), rows // 2)

    def partial_sketch(which, loading):
        left = row_left[half_of(which), :]
        total = None
        for n, at in enumerate(steps):
            if loading:
                loads[2 * n + 1].wait()
            tile = cubed(dot(left, right_terms(col_ref[:, at], 1.0)))
            if loading:
                loads[2 * n + 2].wait()
            share = dot(tile, test_ref[at, :])
            total = share if total is None else total + share
        return total

    pair_send[...] = partial_sketch(1 - half, True).astype(BF16)
    pl.semaphore_wait(barrier, ny + len(around))

    pair = copy(0, pair_send, pair_recv, pair_sem.at[0], sibling)
    pair.start()
    feat = [copy(1, row_ref, rows_recv.at[i - 1], rows_sem.at[i - 1], at_x(i)) for i in range(1, nx)]
    for one in feat:
        one.start()
    partial[...] = partial_sketch(half, False)
    pair.wait_recv()
    partial[...] += pair_recv[...].astype(F32)
    rs_send[...] = partial[...].astype(BF16).reshape(rs_send.shape)
    rs = [copy(2, rs_send.at[lax.rem(y + i, ny)], rs_recv.at[i - 1], rs_sem.at[0], at_y(i)) for i in far_first(ny)]
    for one in rs:
        one.start()
    own = pl.ds(pl.multiple_of(x * per_x, per_x), per_x)
    col_left[...] = left_terms(col_ref[:, own], 1.0)
    total = partial[pl.ds(pl.multiple_of(y * piece, piece), piece), :]
    copy(2, rs_recv, rs_recv, rs_sem.at[0], sibling).wait_recv()
    for i in range(1, ny):
        total = total + rs_recv[i - 1].astype(F32)
    own_sketch[...] = total.astype(BF16)
    sketch[x, place] = own_sketch[...]

    ag = {i: copy(3, own_sketch, sketch.at[x, place], ag_sem.at[i - 1], at_y(i)) for i in far_first(ny)}
    for i in far_first(ny):
        ag[i].start()
    copy(4, own_sketch, sketch.at[x, place], ag2_sem.at[0], sibling).start()
    opposite = nx // 2
    copy(13, own_sketch, sketch.at[x, place], far_sem.at[0], at_x(opposite)).start()

    block = min(256, per_x)
    for i in range(nx):
        if i:
            feat[i - 1].wait_recv()
        source = rows_recv[i - 1] if i else row_ref[...]
        right = right_terms(source, scale)
        at_block = lax.rem(x + nx - i, nx)

        @pl.loop(0, per_x // block)
        def _(m):
            at = pl.ds(pl.multiple_of(m * block, block), block)
            tile_t[at_block, at, :] = cubed(dot(col_left[at, :], right))

    far = lax.rem(x + opposite, nx)
    copy(13, own_sketch, sketch.at[far, place], far_sem.at[0], sibling).wait_recv()
    for i in far_first(ny):
        copy(14, sketch.at[far, place], sketch.at[far, place], far_sem.at[1], at_y(i)).start()

    near_first = far_first(ny)[::-1]
    for i in near_first:
        ag[i].wait_recv()
        there = sketch.at[x, half * ny + lax.rem(y + ny - i, ny)]
        copy(4, there, there, ag2_sem.at[0], sibling).start()
    mine = pl.ds(half * ny, ny)
    other = pl.ds((1 - half) * ny, ny)
    copy(4, sketch.at[x, other], sketch.at[x, other], ag2_sem.at[0], sibling).wait_recv()

    held = sketch[x].reshape(rows, size)
    whole = dot(held, held, ((0,), (0,)))
    top = size // 2
    part = top // nc
    gram[:, 0] = whole[:top, :top].reshape(nc, part, top)
    gram[:, 1] = whole[:top, top:].reshape(nc, part, top)
    gram[:, 2] = whole[top:, top:].reshape(nc, part, top)
    gx = [copy(5, gram.at[place], gx_recv.at[i - 1], gx_sem.at[0], at_x(i)) for i in range(1, nx)]
    for one in gx:
        one.start()
    beside = [i for i in range(1, nx) if i != opposite]
    xag = {i: copy(6, sketch.at[x, mine], sketch.at[x, mine], xag_sem.at[i - 1], at_x(i)) for i in beside}
    for i in beside:
        xag[i].start()
    slice_sum = gram[place]
    copy(5, gx_recv, gx_recv, gx_sem.at[0], sibling).wait_recv()
    for i in range(1, nx):
        slice_sum = slice_sum + gx_recv[i - 1]
    gz_send[...] = slice_sum
    gz = [copy(7, gz_send, gz_recv.at[i - 1], gz_sem.at[0], at_z(i)) for i in far_first(nz)]
    for one in gz:
        one.start()

    copy(14, rs_recv, rs_recv, far_sem.at[1], sibling).wait_recv()
    copy(8, sketch.at[far, mine], sketch.at[far, mine], fwd_sem.at[opposite - 1], sibling).start()
    for i in beside:
        xag[i].wait_recv()
        there = sketch.at[lax.rem(x + nx - i, nx), mine]
        copy(8, there, there, fwd_sem.at[i - 1], sibling).start()
    for i in range(1, nx):
        there = sketch.at[lax.rem(x + nx - i, nx), other]
        copy(8, there, there, fwd_sem.at[i - 1], sibling).wait_recv()

    pairs = nz // 2
    for i in far_first(pairs) + [0]:
        to = lax.rem(z // 2 + i, pairs)
        at = pl.ds(pl.multiple_of(to * 2 * per_z, 2 * per_z), 2 * per_z)
        total = dot(tile_t[0, at, :], sketch[0].reshape(rows, size))
        for j in range(1, nx):
            total = total + dot(tile_t[j, at, :], sketch[j].reshape(rows, size))
        p_send[pl.ds(2 * to, 2)] = total.astype(BF16).reshape(2, per_z, size)
        targets = [2 * to, 2 * to + 1] if i else [z + 1 - 2 * lax.rem(z, 2)]
        for t in targets:
            slot = lax.rem(t + nz - z, nz) - 1
            copy(11, p_send.at[t], p_recv.at[slot], p_sem.at[0], (t * nx + x, c)).start()

    copy(7, gz_recv, gz_recv, gz_sem.at[0], sibling).wait_recv()
    for i in range(1, nz):
        slice_sum = slice_sum + gz_recv[i - 1]
    gy_send[...] = slice_sum
    gram_all[place] = slice_sum
    gy = {i: copy(9, gy_send, gram_all.at[place], gy_sem.at[i - 1], at_y(i)) for i in far_first(ny)}
    for i in far_first(ny):
        gy[i].start()
    copy(10, gy_send, gram_all.at[place], gy2_sem.at[0], sibling).start()

    for i in near_first:
        gy[i].wait_recv()
        there = gram_all.at[half * ny + lax.rem(y + ny - i, ny)]
        copy(10, there, there, gy2_sem.at[0], sibling).start()
    copy(10, gram_all.at[other], gram_all.at[other], gy2_sem.at[0], sibling).wait_recv()
    work[:top, :top] = gram_all[:, 0].reshape(top, top)
    work[:top, top:size] = gram_all[:, 1].reshape(top, top)
    work[top:, :top] = jnp.zeros((top, top), F32)
    work[top:, top:size] = gram_all[:, 2].reshape(top, top)
    diagonal = lax.broadcasted_iota(jnp.int32, (size, size), 0)
    work[:, size:] = jnp.where(diagonal == lax.broadcasted_iota(jnp.int32, (size, size), 1), 1.0, 0.0)
    eliminate(work)

    product = p_send[z].astype(F32)
    copy(11, p_recv, p_recv, p_sem.at[0], sibling).wait_recv()
    for i in range(1, nz):
        product = product + p_recv[i - 1].astype(F32)
    inverse_high, inverse_low = split2(work[:, size:])
    product_high, product_low = split2(product)
    result = dot(
        jnp.concatenate([inverse_high, inverse_high, inverse_low], axis=1),
        jnp.concatenate([product_high, product_low, product_high], axis=1),
        ((1,), (1,)),
    )
    o_send[...] = result.astype(BF16).reshape(o_send.shape)
    spot = x * nz + z
    for i, j in around:
        target = at_zx(i, j)
        copy(12, o_send.at[target[0]], o_recv.at[spot], o_sem.at[0], target).start()
    o_recv[spot] = o_send[r]
    share = size // nc
    take = pl.ds(pl.multiple_of(c * share, share), share)
    share_high, share_low = split2(work[take, size:])
    held = sketch[x].reshape(rows, size)
    basis_ref[...] = dot(share_high, held, ((1,), (1,))) + dot(share_low, held, ((1,), (1,)))
    wait_sent(0, pair_send)
    wait_sent(1, rows_recv)
    wait_sent(2, rs_recv)
    wait_sent(3, rs_recv)
    wait_sent(4, rs_send)
    wait_sent(5, gx_recv)
    if beside:
        wait_sent(6, sketch.at[pl.ds(0, len(beside)), mine])
    wait_sent(7, gz_recv)
    wait_sent(8, sketch.at[pl.ds(0, nx - 1), mine])
    wait_sent(9, gram_all.at[pl.ds(0, ny - 1)])
    wait_sent(10, gram_all.at[mine])
    wait_sent(11, p_recv)
    wait_sent(13, own_sketch)
    wait_sent(14, rs_recv)
    others = o_send.at[pl.ds(0, len(around))]
    copy(12, others, others, o_sem.at[0], sibling).wait()
    for k in range(nx * nz):
        out_ref[:, k * per_z : (k + 1) * per_z] = o_recv[k].astype(F32)


def local(nx, nz, nc, row_features, col_features, test_block):
    rows, width = row_features.shape
    columns, size = test_block.shape
    per_x = columns // nx
    per_z = per_x // nz
    share = size // nc
    piece = rows // nc
    vmem = pltpu.VMEM

    def sems(count):
        return pltpu.SemaphoreType.DMA((count,))

    basis_t, projected = pl.pallas_call(
        functools.partial(kernel, nx, nz, nc),
        out_shape=(
            jax.ShapeDtypeStruct((share, rows), F32),
            jax.ShapeDtypeStruct((size // (nx * nz), columns), F32),
        ),
        in_specs=[pl.BlockSpec(memory_space=pl.ANY)] * 3,
        out_specs=(pl.BlockSpec(memory_space=vmem),) * 2,
        scratch_shapes=[
            vmem((width, rows), F32),
            vmem((width, columns), F32),
            vmem((columns, size), BF16),
            vmem((rows, 3 * width), BF16),
            vmem((per_x, 3 * width), BF16),
            vmem((rows // 2, size), F32),
            vmem((rows // 2, size), BF16),
            vmem((rows // 2, size), BF16),
            vmem((nc // 2, piece, size), BF16),
            vmem((nc // 2 - 1, piece, size), BF16),
            vmem((nx - 1, width, rows), F32),
            vmem((piece, size), BF16),
            vmem((nx, nc, piece, size), BF16),
            vmem((nx, per_x, rows), BF16),
            vmem((nc, 3, size // 2 // nc, size // 2), F32),
            vmem((nx - 1, 3, size // 2 // nc, size // 2), F32),
            vmem((3, size // 2 // nc, size // 2), F32),
            vmem((nz - 1, 3, size // 2 // nc, size // 2), F32),
            vmem((3, size // 2 // nc, size // 2), F32),
            vmem((nc, 3, size // 2 // nc, size // 2), F32),
            vmem((nz, per_z, size), BF16),
            vmem((nz - 1, per_z, size), BF16),
            vmem((size, 2 * size), F32),
            vmem((nx * nz, size // (nx * nz), per_z), BF16),
            vmem((nx * nz, size // (nx * nz), per_z), BF16),
            sems(1 + 2 * STEPS),
            sems(15),
            sems(2),
            sems(nx - 1),
            sems(1),
            sems(1),
            sems(nc // 2 - 1),
            sems(1),
            sems(1),
            sems(nx - 1),
            sems(nx - 1),
            sems(1),
            sems(nc // 2 - 1),
            sems(1),
            sems(1),
            sems(1),
        ],
        compiler_params=pltpu.CompilerParams(
            collective_id=0, has_side_effects=True, vmem_limit_bytes=VMEM_LIMIT
        ),
    )(row_features.T, col_features.T, test_block)
    return basis_t.T, projected


def solution(mesh, nx=ALONG_X):
    nz, nc = mesh.shape["rows"] // nx, mesh.shape["cols"]
    return jax.shard_map(
        functools.partial(local, nx, nz, nc),
        mesh=mesh,
        in_specs=(P("rows", None), P("cols", None), P("cols", None)),
        out_specs=(P("rows", "cols"), P("rows", "cols")),
        check_vma=False,
    )
```

```python
import functools
import math

import jax
import jax.numpy as jnp
from jax import lax
from jax.experimental import pallas as pl
from jax.experimental.pallas import tpu as pltpu
from jax.sharding import PartitionSpec as P

MESH = pl.DeviceIdType.MESH
F32, BF16 = jnp.float32, jnp.bfloat16
ALONG_X = 4
PANEL = 32
PART = 16
ANTIPODE = 4
STEPS = 2
VMEM_LIMIT = 56_300_000


def far_first(length):
    return sorted(range(1, length), key=lambda i: -min(i, length - i))


def split2(v):
    high = v.astype(BF16)
    return high, (v - high.astype(F32)).astype(BF16)


def split3(v):
    high = v.astype(BF16)
    rest = v - high.astype(F32)
    mid = rest.astype(BF16)
    return high, mid, (rest - mid.astype(F32)).astype(BF16)


def dot(a, b, dims=((1,), (0,))):
    return lax.dot_general(a, b, (dims, ((), ())), preferred_element_type=F32)


def cubed(inner):
    shifted = inner + 1.0
    return (shifted * shifted * shifted).astype(BF16)


def left_terms(features_t, scale):
    high, low = split2(features_t * scale)
    return jnp.concatenate([high, high, low], axis=0).T


def right_terms(features_t, scale):
    high, low = split2(features_t * scale)
    return jnp.concatenate([high, low, high], axis=0)


def eliminate(work):
    n = work.shape[0]
    row = lax.broadcasted_iota(jnp.int32, (8, 128), 0)
    groups = PANEL // 8
    for first in range(0, n, PANEL):
        after = first + PANEL
        base = (first // 128) * 128
        offset = first - base
        end = n + ((after + 127) // 128) * 128
        tiles = range(base, end, 128)
        panel = [
            [work[first + 8 * g : first + 8 * g + 8, t : t + 128] for t in tiles] for g in range(groups)
        ]
        for part in range(0, PANEL, PART):
            column = {
                j: {
                    g: jnp.broadcast_to(panel[g][0][:, offset + j : offset + j + 1], (8, 128))
                    for g in range(j // 8, groups)
                }
                for j in range(part, part + PART)
            }
            for k in range(part, part + PART):
                own, at = k // 8, k % 8
                inverse_root = lax.rsqrt(column[k][own][at : at + 1, :])
                lower = {g: v * inverse_root for g, v in column[k].items()}
                for j in range(k + 1, part + PART):
                    factor = lower[j // 8][j % 8 : j % 8 + 1, :]
                    column[j] = {g: v - lower[g] * factor for g, v in column[j].items()}
                below = jnp.where(row > at, lower[own], 0.0)
                for t in range(len(tiles)):
                    pivot_row = panel[own][t][at : at + 1, :] * inverse_root
                    panel[own][t] = jnp.where(
                        row == at,
                        jnp.broadcast_to(pivot_row, (8, 128)),
                        panel[own][t] - below * pivot_row,
                    )
                    for g in range(own + 1, groups):
                        panel[g][t] = panel[g][t] - lower[g] * pivot_row
        panel = jnp.concatenate([jnp.concatenate(g, axis=1) for g in panel], axis=0)
        work[first:after, base:end] = panel
        if after < n:
            high, mid, low = split3(panel)
            start = (after // 128) * 128
            keep = slice(start - base, n - base)
            left = jnp.concatenate([t[:, keep] for t in (high, high, mid, high, mid, low)], axis=0)
            right = jnp.concatenate([high, mid, high, low, mid, high], axis=0)
            work[after:, base:end] = work[after:, base:end] - dot(left.T[after - start :, :], right)


def kernel(
    nx, nz, nc,
    row_hbm, col_hbm, test_hbm, basis_ref, out_ref,
    row_ref, col_ref, test_ref,
    row_left, col_left, partial, pair_send, pair_recv, rs_send, rs_recv, rows_recv, own_sketch, sketch,
    tile_t, gram, gx_recv, gz_send, gz_recv, gy_send, gram_all,
    p_send, p_recv, relay_recv, work, o_send, o_recv,
    in_sem, sent_sem, far_sem, rows_sem, pair_sem, rs_sem, ag_sem, ag2_sem, gx_sem, xag_sem, fwd_sem, gz_sem, gy_sem, gy2_sem,
    p_sem, o_sem,
):
    r, c = lax.axis_index("rows"), lax.axis_index("cols")
    z, x = r // nx, lax.rem(r, nx)
    ny = nc // 2
    y, half = c // 2, lax.rem(c, 2)
    rows, size = 2 * partial.shape[0], partial.shape[1]
    piece = rows // nc
    width = row_ref.shape[0]
    scale = 1.0 / math.sqrt(width)
    columns = col_ref.shape[1]
    per_x = columns // nx
    per_z = per_x // nz
    place = half * ny + y

    def at_x(i):
        return (z * nx + lax.rem(x + i, nx), c)

    def at_z(i):
        return (lax.rem(z + i, nz) * nx + x, c)

    def at_y(i):
        return (r, lax.rem(y + i, ny) * 2 + half)

    def at_zx(i, j):
        return (lax.rem(z + i, nz) * nx + lax.rem(x + j, nx), c)

    sibling = (r, c + 1 - 2 * half)
    around = [(i, j) for i in range(nz) for j in range(nx) if (i, j) != (0, 0)]
    around.sort(key=lambda ij: -min(ij[0], nz - ij[0]) - min(ij[1], nx - ij[1]))

    def copy(group, src, dst, recv_sem, device):
        return pltpu.make_async_remote_copy(
            src_ref=src,
            dst_ref=dst,
            send_sem=sent_sem.at[group],
            recv_sem=recv_sem,
            device_id=device,
            device_id_type=MESH,
        )

    def wait_sent(group, whole):
        copy(group, whole, whole, in_sem.at[0], sibling).wait_send()

    steps = [slice(n, n + columns // STEPS) for n in range(0, columns, columns // STEPS)]
    pieces = [(row_hbm, row_ref)]
    for at in steps:
        pieces += [(col_hbm.at[:, at], col_ref.at[:, at]), (test_hbm.at[at, :], test_ref.at[at, :])]
    loads = [pltpu.make_async_copy(src, dst, in_sem.at[k]) for k, (src, dst) in enumerate(pieces)]
    for one in loads:
        one.start()
    barrier = pltpu.get_barrier_semaphore()
    for i, j in around:
        pl.semaphore_signal(barrier, inc=1, device_id=at_zx(i, j), device_id_type=MESH)
    for i in far_first(ny):
        pl.semaphore_signal(barrier, inc=1, device_id=at_y(i), device_id_type=MESH)
    pl.semaphore_signal(barrier, inc=1, device_id=sibling, device_id_type=MESH)

    loads[0].wait()
    row_left[...] = left_terms(row_ref[...], scale)
    def half_of(which):
        return pl.ds(pl.multiple_of(which * (rows // 2), rows // 2), rows // 2)

    def partial_sketch(which, n, loading):
        left = row_left[half_of(which), :]
        at = steps[n]
        if loading:
            loads[2 * n + 1].wait()
        tile = cubed(dot(left, right_terms(col_ref[:, at], 1.0)))
        if loading:
            loads[2 * n + 2].wait()
        return dot(tile, test_ref[at, :])

    theirs = partial_sketch(1 - half, 0, True)
    for n in range(1, STEPS):
        theirs = theirs + partial_sketch(1 - half, n, True)
    pair_send[...] = theirs.astype(BF16)
    ours = partial_sketch(half, 0, False)
    for n in range(1, STEPS // 2):
        ours = ours + partial_sketch(half, n, False)
    partial[...] = ours
    pl.semaphore_wait(barrier, ny + len(around))

    pair = copy(0, pair_send, pair_recv, pair_sem.at[0], sibling)
    pair.start()
    feat = [copy(1, row_ref, rows_recv.at[i - 1], rows_sem.at[i - 1], at_x(i)) for i in range(1, nx)]
    for one in feat:
        one.start()
    for n in range(STEPS // 2, STEPS):
        partial[...] += partial_sketch(half, n, False)
    pair.wait_recv()
    partial[...] += pair_recv[...].astype(F32)
    rs_send[...] = partial[...].astype(BF16).reshape(rs_send.shape)
    rs = [copy(2, rs_send.at[lax.rem(y + i, ny)], rs_recv.at[i - 1], rs_sem.at[0], at_y(i)) for i in far_first(ny)]
    for one in rs:
        one.start()
    own = pl.ds(pl.multiple_of(x * per_x, per_x), per_x)
    col_left[...] = left_terms(col_ref[:, own], 1.0)
    total = partial[pl.ds(pl.multiple_of(y * piece, piece), piece), :]
    copy(2, rs_recv, rs_recv, rs_sem.at[0], sibling).wait_recv()
    for i in range(1, ny):
        total = total + rs_recv[i - 1].astype(F32)
    own_sketch[...] = total.astype(BF16)
    sketch[x, place] = own_sketch[...]

    ag = {i: copy(3, own_sketch, sketch.at[x, place], ag_sem.at[i - 1], at_y(i)) for i in far_first(ny)}
    for i in far_first(ny):
        ag[i].start()
    copy(4, own_sketch, sketch.at[x, place], ag2_sem.at[0], sibling).start()
    opposite = nx // 2
    copy(13, own_sketch, sketch.at[x, place], far_sem.at[0], at_x(opposite)).start()

    block = min(256, per_x)
    for i in range(nx):
        if i:
            feat[i - 1].wait_recv()
        source = rows_recv[i - 1] if i else row_ref[...]
        right = right_terms(source, scale)
        at_block = lax.rem(x + nx - i, nx)

        @pl.loop(0, per_x // block)
        def _(m):
            at = pl.ds(pl.multiple_of(m * block, block), block)
            tile_t[at_block, at, :] = cubed(dot(col_left[at, :], right))

    far = lax.rem(x + opposite, nx)
    copy(13, own_sketch, sketch.at[far, place], far_sem.at[0], sibling).wait_recv()
    for i in far_first(ny):
        copy(14, sketch.at[far, place], sketch.at[far, place], far_sem.at[1], at_y(i)).start()

    near_first = far_first(ny)[::-1]
    for i in near_first:
        ag[i].wait_recv()
        there = sketch.at[x, half * ny + lax.rem(y + ny - i, ny)]
        copy(4, there, there, ag2_sem.at[0], sibling).start()
    mine = pl.ds(half * ny, ny)
    other = pl.ds((1 - half) * ny, ny)
    copy(4, sketch.at[x, other], sketch.at[x, other], ag2_sem.at[0], sibling).wait_recv()

    held = sketch[x].reshape(rows, size)
    whole = dot(held, held, ((0,), (0,)))
    top = size // 2
    part = top // nc
    gram[:, 0] = whole[:top, :top].reshape(nc, part, top)
    gram[:, 1] = whole[:top, top:].reshape(nc, part, top)
    gram[:, 2] = whole[top:, top:].reshape(nc, part, top)
    gx = [copy(5, gram.at[place], gx_recv.at[i - 1], gx_sem.at[0], at_x(i)) for i in range(1, nx)]
    for one in gx:
        one.start()
    beside = [i for i in range(1, nx) if i != opposite]
    xag = {i: copy(6, sketch.at[x, mine], sketch.at[x, mine], xag_sem.at[i - 1], at_x(i)) for i in beside}
    for i in beside:
        xag[i].start()
    slice_sum = gram[place]
    copy(5, gx_recv, gx_recv, gx_sem.at[0], sibling).wait_recv()
    for i in range(1, nx):
        slice_sum = slice_sum + gx_recv[i - 1]
    gz_send[...] = slice_sum
    gz = [copy(7, gz_send, gz_recv.at[i - 1], gz_sem.at[0], at_z(i)) for i in far_first(nz)]
    for one in gz:
        one.start()

    copy(14, rs_recv, rs_recv, far_sem.at[1], sibling).wait_recv()
    copy(8, sketch.at[far, mine], sketch.at[far, mine], fwd_sem.at[opposite - 1], sibling).start()
    for i in beside:
        xag[i].wait_recv()
        there = sketch.at[lax.rem(x + nx - i, nx), mine]
        copy(8, there, there, fwd_sem.at[i - 1], sibling).start()
    for i in range(1, nx):
        there = sketch.at[lax.rem(x + nx - i, nx), other]
        copy(8, there, there, fwd_sem.at[i - 1], sibling).wait_recv()

    pairs = nz // 2

    def form(i):
        to = lax.rem(z // 2 + i, pairs)
        at = pl.ds(pl.multiple_of(to * 2 * per_z, 2 * per_z), 2 * per_z)
        total = dot(tile_t[0, at, :], sketch[0].reshape(rows, size))
        for j in range(1, nx):
            total = total + dot(tile_t[j, at, :], sketch[j].reshape(rows, size))
        p_send[pl.ds(2 * to, 2)] = total.astype(BF16).reshape(2, per_z, size)

    def send(*distances):
        for d in distances:
            slot = d - 1 if d < ANTIPODE or nz <= ANTIPODE else d - 2
            copy(11, p_send.at[lax.rem(z + d, nz)], p_recv.at[slot], p_sem.at[0], at_z(d)).start()

    relayed = nz == 2 * ANTIPODE
    if relayed:
        form(2)
        relay = copy(15, p_send.at[lax.rem(z + ANTIPODE, nz)], relay_recv, p_sem.at[1], at_z(nz - 1))
        relay.start()
        form(3)
        send(6)
        form(1)
        send(3, 2)

    copy(7, gz_recv, gz_recv, gz_sem.at[0], sibling).wait_recv()
    for i in range(1, nz):
        slice_sum = slice_sum + gz_recv[i - 1]
    gy_send[...] = slice_sum
    gram_all[place] = slice_sum
    gy = {i: copy(9, gy_send, gram_all.at[place], gy_sem.at[i - 1], at_y(i)) for i in far_first(ny)}
    for i in far_first(ny):
        gy[i].start()
    copy(10, gy_send, gram_all.at[place], gy2_sem.at[0], sibling).start()

    if relayed:
        form(0)
        send(7, 1)
    else:
        for i in range(pairs):
            form(i)
        send(*far_first(nz))

    for i in near_first:
        gy[i].wait_recv()
        there = gram_all.at[half * ny + lax.rem(y + ny - i, ny)]
        copy(10, there, there, gy2_sem.at[0], sibling).start()
    if relayed:
        relay.wait_recv()
        joint = lax.rem(z + 5, nz)
        p_send[joint] = (p_send[joint].astype(F32) + relay_recv[...].astype(F32)).astype(BF16)
        send(5)
    copy(10, gram_all.at[other], gram_all.at[other], gy2_sem.at[0], sibling).wait_recv()
    work[:top, :top] = gram_all[:, 0].reshape(top, top)
    work[:top, top:size] = gram_all[:, 1].reshape(top, top)
    work[top:, :top] = jnp.zeros((top, top), F32)
    work[top:, top:size] = gram_all[:, 2].reshape(top, top)
    diagonal = lax.broadcasted_iota(jnp.int32, (size, size), 0)
    work[:, size:] = jnp.where(diagonal == lax.broadcasted_iota(jnp.int32, (size, size), 1), 1.0, 0.0)
    eliminate(work)

    product = p_send[z].astype(F32)
    copy(11, p_recv, p_recv, p_sem.at[0], sibling).wait_recv()
    for i in range(p_recv.shape[0]):
        product = product + p_recv[i].astype(F32)
    inverse_high, inverse_low = split2(work[:, size:])
    product_high, product_low = split2(product)
    result = dot(
        jnp.concatenate([inverse_high, inverse_high, inverse_low], axis=1),
        jnp.concatenate([product_high, product_low, product_high], axis=1),
        ((1,), (1,)),
    )
    o_send[...] = result.astype(BF16).reshape(o_send.shape)
    spot = x * nz + z
    for i, j in around:
        target = at_zx(i, j)
        copy(12, o_send.at[target[0]], o_recv.at[spot], o_sem.at[0], target).start()
    o_recv[spot] = o_send[r]
    share = size // nc
    take = pl.ds(pl.multiple_of(c * share, share), share)
    share_high, share_low = split2(work[take, size:])
    held = sketch[x].reshape(rows, size)
    basis_ref[...] = dot(share_high, held, ((1,), (1,))) + dot(share_low, held, ((1,), (1,)))
    wait_sent(0, pair_send)
    wait_sent(1, rows_recv)
    wait_sent(2, rs_recv)
    wait_sent(3, rs_recv)
    wait_sent(4, rs_send)
    wait_sent(5, gx_recv)
    if beside:
        wait_sent(6, sketch.at[pl.ds(0, len(beside)), mine])
    wait_sent(7, gz_recv)
    wait_sent(8, sketch.at[pl.ds(0, nx - 1), mine])
    wait_sent(9, gram_all.at[pl.ds(0, ny - 1)])
    wait_sent(10, gram_all.at[mine])
    wait_sent(11, p_recv)
    wait_sent(13, own_sketch)
    wait_sent(14, rs_recv)
    if relayed:
        wait_sent(15, relay_recv)
    others = o_send.at[pl.ds(0, len(around))]
    copy(12, others, others, o_sem.at[0], sibling).wait()
    for k in range(nx * nz):
        out_ref[:, k * per_z : (k + 1) * per_z] = o_recv[k].astype(F32)


def local(nx, nz, nc, row_features, col_features, test_block):
    rows, width = row_features.shape
    columns, size = test_block.shape
    per_x = columns // nx
    per_z = per_x // nz
    share = size // nc
    piece = rows // nc
    vmem = pltpu.VMEM

    def sems(count):
        return pltpu.SemaphoreType.DMA((count,))

    basis_t, projected = pl.pallas_call(
        functools.partial(kernel, nx, nz, nc),
        out_shape=(
            jax.ShapeDtypeStruct((share, rows), F32),
            jax.ShapeDtypeStruct((size // (nx * nz), columns), F32),
        ),
        in_specs=[pl.BlockSpec(memory_space=pl.ANY)] * 3,
        out_specs=(pl.BlockSpec(memory_space=vmem),) * 2,
        scratch_shapes=[
            vmem((width, rows), F32),
            vmem((width, columns), F32),
            vmem((columns, size), BF16),
            vmem((rows, 3 * width), BF16),
            vmem((per_x, 3 * width), BF16),
            vmem((rows // 2, size), F32),
            vmem((rows // 2, size), BF16),
            vmem((rows // 2, size), BF16),
            vmem((nc // 2, piece, size), BF16),
            vmem((nc // 2 - 1, piece, size), BF16),
            vmem((nx - 1, width, rows), F32),
            vmem((piece, size), BF16),
            vmem((nx, nc, piece, size), BF16),
            vmem((nx, per_x, rows), BF16),
            vmem((nc, 3, size // 2 // nc, size // 2), F32),
            vmem((nx - 1, 3, size // 2 // nc, size // 2), F32),
            vmem((3, size // 2 // nc, size // 2), F32),
            vmem((nz - 1, 3, size // 2 // nc, size // 2), F32),
            vmem((3, size // 2 // nc, size // 2), F32),
            vmem((nc, 3, size // 2 // nc, size // 2), F32),
            vmem((nz, per_z, size), BF16),
            vmem((nz - 2 if nz == 2 * ANTIPODE else nz - 1, per_z, size), BF16),
            vmem((per_z, size), BF16),
            vmem((size, 2 * size), F32),
            vmem((nx * nz, size // (nx * nz), per_z), BF16),
            vmem((nx * nz, size // (nx * nz), per_z), BF16),
            sems(1 + 2 * STEPS),
            sems(16),
            sems(2),
            sems(nx - 1),
            sems(1),
            sems(1),
            sems(nc // 2 - 1),
            sems(1),
            sems(1),
            sems(nx - 1),
            sems(nx - 1),
            sems(1),
            sems(nc // 2 - 1),
            sems(1),
            sems(2),
            sems(1),
        ],
        compiler_params=pltpu.CompilerParams(
            collective_id=0, has_side_effects=True, vmem_limit_bytes=VMEM_LIMIT
        ),
    )(row_features.T, col_features.T, test_block)
    return basis_t.T, projected


def solution(mesh, nx=ALONG_X):
    nz, nc = mesh.shape["rows"] // nx, mesh.shape["cols"]
    return jax.shard_map(
        functools.partial(local, nx, nz, nc),
        mesh=mesh,
        in_specs=(P("rows", None), P("cols", None), P("cols", None)),
        out_specs=(P("rows", "cols"), P("rows", "cols")),
        check_vma=False,
    )
```

```python
import functools
import math

import jax
import jax.numpy as jnp
from jax import lax
from jax.experimental import pallas as pl
from jax.experimental.pallas import tpu as pltpu
from jax.sharding import PartitionSpec as P

MESH = pl.DeviceIdType.MESH
F32, BF16 = jnp.float32, jnp.bfloat16
ALONG_X = 4
PANEL = 32
PART = 16
ANTIPODE = 4
STEPS = 2
VMEM_LIMIT = 56_400_000


def far_first(length):
    return sorted(range(1, length), key=lambda i: -min(i, length - i))


def split2(v):
    high = v.astype(BF16)
    return high, (v - high.astype(F32)).astype(BF16)


def split3(v):
    high = v.astype(BF16)
    rest = v - high.astype(F32)
    mid = rest.astype(BF16)
    return high, mid, (rest - mid.astype(F32)).astype(BF16)


def dot(a, b, dims=((1,), (0,))):
    return lax.dot_general(a, b, (dims, ((), ())), preferred_element_type=F32)


def cubed(inner):
    shifted = inner + 1.0
    return (shifted * shifted * shifted).astype(BF16)


def left_terms(features_t, scale):
    high, low = split2(features_t * scale)
    return jnp.concatenate([high, high, low], axis=0).T


def right_terms(features_t, scale):
    high, low = split2(features_t * scale)
    return jnp.concatenate([high, low, high], axis=0)


def eliminate(work):
    n = work.shape[0]
    row = lax.broadcasted_iota(jnp.int32, (8, 128), 0)
    groups = PANEL // 8
    for first in range(0, n, PANEL):
        after = first + PANEL
        base = (first // 128) * 128
        offset = first - base
        end = n + ((after + 127) // 128) * 128
        tiles = range(base, end, 128)
        panel = [
            [work[first + 8 * g : first + 8 * g + 8, t : t + 128] for t in tiles] for g in range(groups)
        ]
        for part in range(0, PANEL, PART):
            column = {
                j: {
                    g: jnp.broadcast_to(panel[g][0][:, offset + j : offset + j + 1], (8, 128))
                    for g in range(j // 8, groups)
                }
                for j in range(part, part + PART)
            }
            for k in range(part, part + PART):
                own, at = k // 8, k % 8
                inverse_root = lax.rsqrt(column[k][own][at : at + 1, :])
                lower = {g: v * inverse_root for g, v in column[k].items()}
                for j in range(k + 1, part + PART):
                    factor = lower[j // 8][j % 8 : j % 8 + 1, :]
                    column[j] = {g: v - lower[g] * factor for g, v in column[j].items()}
                below = jnp.where(row > at, lower[own], 0.0)
                for t in range(len(tiles)):
                    pivot_row = panel[own][t][at : at + 1, :] * inverse_root
                    panel[own][t] = jnp.where(
                        row == at,
                        jnp.broadcast_to(pivot_row, (8, 128)),
                        panel[own][t] - below * pivot_row,
                    )
                    for g in range(own + 1, groups):
                        panel[g][t] = panel[g][t] - lower[g] * pivot_row
        panel = jnp.concatenate([jnp.concatenate(g, axis=1) for g in panel], axis=0)
        work[first:after, base:end] = panel
        if after < n:
            high, mid, low = split3(panel)
            start = (after // 128) * 128
            keep = slice(start - base, n - base)
            left = jnp.concatenate([t[:, keep] for t in (high, high, mid, high, mid, low)], axis=0)
            right = jnp.concatenate([high, mid, high, low, mid, high], axis=0)
            work[after:, base:end] = work[after:, base:end] - dot(left.T[after - start :, :], right)


def kernel(
    nx, nz, nc,
    row_hbm, col_hbm, test_hbm, basis_ref, out_ref,
    row_ref, col_ref, test_ref,
    row_left, col_left, partial, pair_send, pair_recv, rs_send, rs_recv, rows_recv, own_sketch, sketch,
    tile_t, gram, gx_recv, gz_send, gz_recv, gy_send, gram_all,
    p_send, p_recv, relay_recv, work, o_send, o_recv,
    in_sem, sent_sem, far_sem, rows_sem, pair_sem, rs_sem, ag_sem, ag2_sem, gx_sem, xag_sem, fwd_sem, gz_sem, gy_sem, gy2_sem,
    p_sem, o_sem,
):
    r, c = lax.axis_index("rows"), lax.axis_index("cols")
    z, x = r // nx, lax.rem(r, nx)
    ny = nc // 2
    y, half = c // 2, lax.rem(c, 2)
    rows, size = 2 * partial.shape[0], partial.shape[1]
    piece = rows // nc
    width = row_ref.shape[0]
    scale = 1.0 / math.sqrt(width)
    columns = col_ref.shape[1]
    per_x = columns // nx
    per_z = per_x // nz
    place = half * ny + y

    def at_x(i):
        return (z * nx + lax.rem(x + i, nx), c)

    def at_z(i):
        return (lax.rem(z + i, nz) * nx + x, c)

    def at_y(i):
        return (r, lax.rem(y + i, ny) * 2 + half)

    def at_zx(i, j):
        return (lax.rem(z + i, nz) * nx + lax.rem(x + j, nx), c)

    sibling = (r, c + 1 - 2 * half)
    around = [(i, j) for i in range(nz) for j in range(nx) if (i, j) != (0, 0)]
    around.sort(key=lambda ij: -min(ij[0], nz - ij[0]) - min(ij[1], nx - ij[1]))

    def copy(group, src, dst, recv_sem, device):
        return pltpu.make_async_remote_copy(
            src_ref=src,
            dst_ref=dst,
            send_sem=sent_sem.at[group],
            recv_sem=recv_sem,
            device_id=device,
            device_id_type=MESH,
        )

    def wait_sent(group, whole):
        copy(group, whole, whole, in_sem.at[0], sibling).wait_send()

    steps = [slice(n, n + columns // STEPS) for n in range(0, columns, columns // STEPS)]
    pieces = [(row_hbm, row_ref)]
    for at in steps:
        pieces += [(col_hbm.at[:, at], col_ref.at[:, at]), (test_hbm.at[at, :], test_ref.at[at, :])]
    loads = [pltpu.make_async_copy(src, dst, in_sem.at[k]) for k, (src, dst) in enumerate(pieces)]
    for one in loads:
        one.start()
    barrier = pltpu.get_barrier_semaphore()
    for i, j in around:
        pl.semaphore_signal(barrier, inc=1, device_id=at_zx(i, j), device_id_type=MESH)
    for i in far_first(ny):
        pl.semaphore_signal(barrier, inc=1, device_id=at_y(i), device_id_type=MESH)
    pl.semaphore_signal(barrier, inc=1, device_id=sibling, device_id_type=MESH)

    loads[0].wait()
    row_left[...] = left_terms(row_ref[...], scale)
    def half_of(which):
        return pl.ds(pl.multiple_of(which * (rows // 2), rows // 2), rows // 2)

    def partial_sketch(which, n, loading):
        left = row_left[half_of(which), :]
        at = steps[n]
        if loading:
            loads[2 * n + 1].wait()
        tile = cubed(dot(left, right_terms(col_ref[:, at], 1.0)))
        if loading:
            loads[2 * n + 2].wait()
        return dot(tile, test_ref[at, :])

    theirs = partial_sketch(1 - half, 0, True)
    for n in range(1, STEPS):
        theirs = theirs + partial_sketch(1 - half, n, True)
    pair_send[...] = theirs.astype(BF16)
    ours = partial_sketch(half, 0, False)
    for n in range(1, STEPS // 2):
        ours = ours + partial_sketch(half, n, False)
    partial[...] = ours
    pl.semaphore_wait(barrier, ny + len(around))

    pair = copy(0, pair_send, pair_recv, pair_sem.at[0], sibling)
    pair.start()
    feat = [copy(1, row_ref, rows_recv.at[i - 1], rows_sem.at[i - 1], at_x(i)) for i in range(1, nx)]
    for one in feat:
        one.start()
    for n in range(STEPS // 2, STEPS):
        partial[...] += partial_sketch(half, n, False)
    pair.wait_recv()
    partial[...] += pair_recv[...].astype(F32)
    rs_send[...] = partial[...].astype(BF16).reshape(rs_send.shape)
    rs = [copy(2, rs_send.at[lax.rem(y + i, ny)], rs_recv.at[i - 1], rs_sem.at[0], at_y(i)) for i in far_first(ny)]
    for one in rs:
        one.start()
    own = pl.ds(pl.multiple_of(x * per_x, per_x), per_x)
    col_left[...] = left_terms(col_ref[:, own], 1.0)
    total = partial[pl.ds(pl.multiple_of(y * piece, piece), piece), :]
    copy(2, rs_recv, rs_recv, rs_sem.at[0], sibling).wait_recv()
    for i in range(1, ny):
        total = total + rs_recv[i - 1].astype(F32)
    own_sketch[...] = total.astype(BF16)
    sketch[x, place] = own_sketch[...]

    ag = {i: copy(3, own_sketch, sketch.at[x, place], ag_sem.at[i - 1], at_y(i)) for i in far_first(ny)}
    for i in far_first(ny):
        ag[i].start()
    copy(4, own_sketch, sketch.at[x, place], ag2_sem.at[0], sibling).start()
    opposite = nx // 2
    copy(13, own_sketch, sketch.at[x, place], far_sem.at[0], at_x(opposite)).start()

    block = min(256, per_x)
    for i in range(nx):
        if i:
            feat[i - 1].wait_recv()
        source = rows_recv[i - 1] if i else row_ref[...]
        right = right_terms(source, scale)
        at_block = lax.rem(x + nx - i, nx)

        @pl.loop(0, per_x // block)
        def _(m):
            at = pl.ds(pl.multiple_of(m * block, block), block)
            tile_t[at_block, at, :] = cubed(dot(col_left[at, :], right))

    far = lax.rem(x + opposite, nx)
    copy(13, own_sketch, sketch.at[far, place], far_sem.at[0], sibling).wait_recv()
    for i in far_first(ny):
        copy(14, sketch.at[far, place], sketch.at[far, place], far_sem.at[1], at_y(i)).start()

    near_first = far_first(ny)[::-1]
    for i in near_first:
        ag[i].wait_recv()
        there = sketch.at[x, half * ny + lax.rem(y + ny - i, ny)]
        copy(4, there, there, ag2_sem.at[0], sibling).start()
    mine = pl.ds(half * ny, ny)
    other = pl.ds((1 - half) * ny, ny)
    copy(4, sketch.at[x, other], sketch.at[x, other], ag2_sem.at[0], sibling).wait_recv()

    held = sketch[x].reshape(rows, size)
    whole = dot(held, held, ((0,), (0,)))
    top = size // 2
    part = top // nc
    gram[:, 0] = whole[:top, :top].reshape(nc, part, top)
    gram[:, 1] = whole[:top, top:].reshape(nc, part, top)
    gram[:, 2] = whole[top:, top:].reshape(nc, part, top)
    gx = [copy(5, gram.at[place], gx_recv.at[i - 1], gx_sem.at[0], at_x(i)) for i in range(1, nx)]
    for one in gx:
        one.start()
    beside = [i for i in range(1, nx) if i != opposite]
    xag = {i: copy(6, sketch.at[x, mine], sketch.at[x, mine], xag_sem.at[i - 1], at_x(i)) for i in beside}
    for i in beside:
        xag[i].start()
    slice_sum = gram[place]
    copy(5, gx_recv, gx_recv, gx_sem.at[0], sibling).wait_recv()
    for i in range(1, nx):
        slice_sum = slice_sum + gx_recv[i - 1]
    gz_send[...] = slice_sum
    gz = [copy(7, gz_send, gz_recv.at[i - 1], gz_sem.at[0], at_z(i)) for i in far_first(nz)]
    for one in gz:
        one.start()

    copy(14, rs_recv, rs_recv, far_sem.at[1], sibling).wait_recv()
    copy(8, sketch.at[far, mine], sketch.at[far, mine], fwd_sem.at[opposite - 1], sibling).start()
    for i in beside:
        xag[i].wait_recv()
        there = sketch.at[lax.rem(x + nx - i, nx), mine]
        copy(8, there, there, fwd_sem.at[i - 1], sibling).start()
    for i in range(1, nx):
        there = sketch.at[lax.rem(x + nx - i, nx), other]
        copy(8, there, there, fwd_sem.at[i - 1], sibling).wait_recv()

    pairs = nz // 2

    def form(i):
        to = lax.rem(z // 2 + i, pairs)
        at = pl.ds(pl.multiple_of(to * 2 * per_z, 2 * per_z), 2 * per_z)
        total = dot(tile_t[0, at, :], sketch[0].reshape(rows, size))
        for j in range(1, nx):
            total = total + dot(tile_t[j, at, :], sketch[j].reshape(rows, size))
        p_send[pl.ds(2 * to, 2)] = total.astype(BF16).reshape(2, per_z, size)

    def send(*distances):
        for d in distances:
            slot = d - 1 if d < ANTIPODE or nz <= ANTIPODE else d - 2
            copy(11, p_send.at[lax.rem(z + d, nz)], p_recv.at[slot], p_sem.at[0], at_z(d)).start()

    relayed = nz == 2 * ANTIPODE
    if relayed:
        form(2)
        relay = copy(15, p_send.at[lax.rem(z + ANTIPODE, nz)], relay_recv, p_sem.at[1], at_z(nz - 1))
        relay.start()
        form(3)
        send(6)
        form(1)
        send(3, 2)

    copy(7, gz_recv, gz_recv, gz_sem.at[0], sibling).wait_recv()
    for i in range(1, nz):
        slice_sum = slice_sum + gz_recv[i - 1]
    gy_send[...] = slice_sum
    gram_all[place] = slice_sum
    gy = {i: copy(9, gy_send, gram_all.at[place], gy_sem.at[i - 1], at_y(i)) for i in far_first(ny)}
    for i in far_first(ny):
        gy[i].start()
    copy(10, gy_send, gram_all.at[place], gy2_sem.at[0], sibling).start()

    if relayed:
        form(0)
        send(7, 1)
    else:
        for i in range(pairs):
            form(i)
        send(*far_first(nz))

    for i in near_first:
        gy[i].wait_recv()
        there = gram_all.at[half * ny + lax.rem(y + ny - i, ny)]
        copy(10, there, there, gy2_sem.at[0], sibling).start()
    if relayed:
        relay.wait_recv()
        joint = lax.rem(z + 5, nz)
        p_send[joint] = (p_send[joint].astype(F32) + relay_recv[...].astype(F32)).astype(BF16)
        send(5)
    copy(10, gram_all.at[other], gram_all.at[other], gy2_sem.at[0], sibling).wait_recv()
    work[:top, :top] = gram_all[:, 0].reshape(top, top)
    work[:top, top:size] = gram_all[:, 1].reshape(top, top)
    work[top:, :top] = jnp.zeros((top, top), F32)
    work[top:, top:size] = gram_all[:, 2].reshape(top, top)
    diagonal = lax.broadcasted_iota(jnp.int32, (size, size), 0)
    work[:, size:] = jnp.where(diagonal == lax.broadcasted_iota(jnp.int32, (size, size), 1), 1.0, 0.0)
    eliminate(work)

    product = p_send[z].astype(F32)
    copy(11, p_recv, p_recv, p_sem.at[0], sibling).wait_recv()
    for i in range(p_recv.shape[0]):
        product = product + p_recv[i].astype(F32)
    inverse_high, inverse_low = split2(work[:, size:])
    product_high, product_low = split2(product)
    result = dot(
        jnp.concatenate([inverse_high, inverse_high, inverse_low], axis=1),
        jnp.concatenate([product_high, product_low, product_high], axis=1),
        ((1,), (1,)),
    )
    o_send[...] = result.astype(BF16).reshape(o_send.shape)
    spot = x * nz + z
    for i, j in around:
        target = at_zx(i, j)
        copy(12, o_send.at[target[0]], o_recv.at[spot], o_sem.at[0], target).start()
    o_recv[spot] = o_send[r]
    share = size // nc
    take = pl.ds(pl.multiple_of(c * share, share), share)
    share_high, share_low = split2(work[take, size:])
    held = sketch[x].reshape(rows, size)
    basis_ref[...] = dot(share_high, held, ((1,), (1,))) + dot(share_low, held, ((1,), (1,)))
    wait_sent(0, pair_send)
    wait_sent(1, rows_recv)
    wait_sent(2, rs_recv)
    wait_sent(3, rs_recv)
    wait_sent(4, rs_send)
    wait_sent(5, gx_recv)
    if beside:
        wait_sent(6, sketch.at[pl.ds(0, len(beside)), mine])
    wait_sent(7, gz_recv)
    wait_sent(8, sketch.at[pl.ds(0, nx - 1), mine])
    wait_sent(9, gram_all.at[pl.ds(0, ny - 1)])
    wait_sent(10, gram_all.at[mine])
    wait_sent(11, p_recv)
    wait_sent(13, own_sketch)
    wait_sent(14, rs_recv)
    if relayed:
        wait_sent(15, relay_recv)
    others = o_send.at[pl.ds(0, len(around))]
    copy(12, others, others, o_sem.at[0], sibling).wait()
    out_ref[...] = o_recv[...]


def finish(basis_ref, pieces_ref, basis_hbm, out_hbm, out_ref, sem):
    basis = pltpu.make_async_copy(basis_ref, basis_hbm, sem.at[0])
    basis.start()
    width = pieces_ref.shape[2]
    for k in range(pieces_ref.shape[0]):
        out_ref[:, k * width : (k + 1) * width] = pieces_ref[k].astype(F32)
    out = pltpu.make_async_copy(out_ref, out_hbm, sem.at[1])
    out.start()
    basis.wait()
    out.wait()


def local(nx, nz, nc, row_features, col_features, test_block):
    rows, width = row_features.shape
    columns, size = test_block.shape
    per_x = columns // nx
    per_z = per_x // nz
    share = size // nc
    piece = rows // nc
    vmem = pltpu.VMEM

    def sems(count):
        return pltpu.SemaphoreType.DMA((count,))

    basis_t, pieces = pl.pallas_call(
        functools.partial(kernel, nx, nz, nc),
        out_shape=(
            jax.ShapeDtypeStruct((share, rows), F32),
            jax.ShapeDtypeStruct((nx * nz, size // (nx * nz), per_z), BF16),
        ),
        in_specs=[pl.BlockSpec(memory_space=pl.ANY)] * 3,
        out_specs=(pl.BlockSpec(memory_space=vmem),) * 2,
        scratch_shapes=[
            vmem((width, rows), F32),
            vmem((width, columns), F32),
            vmem((columns, size), BF16),
            vmem((rows, 3 * width), BF16),
            vmem((per_x, 3 * width), BF16),
            vmem((rows // 2, size), F32),
            vmem((rows // 2, size), BF16),
            vmem((rows // 2, size), BF16),
            vmem((nc // 2, piece, size), BF16),
            vmem((nc // 2 - 1, piece, size), BF16),
            vmem((nx - 1, width, rows), F32),
            vmem((piece, size), BF16),
            vmem((nx, nc, piece, size), BF16),
            vmem((nx, per_x, rows), BF16),
            vmem((nc, 3, size // 2 // nc, size // 2), F32),
            vmem((nx - 1, 3, size // 2 // nc, size // 2), F32),
            vmem((3, size // 2 // nc, size // 2), F32),
            vmem((nz - 1, 3, size // 2 // nc, size // 2), F32),
            vmem((3, size // 2 // nc, size // 2), F32),
            vmem((nc, 3, size // 2 // nc, size // 2), F32),
            vmem((nz, per_z, size), BF16),
            vmem((nz - 2 if nz == 2 * ANTIPODE else nz - 1, per_z, size), BF16),
            vmem((per_z, size), BF16),
            vmem((size, 2 * size), F32),
            vmem((nx * nz, size // (nx * nz), per_z), BF16),
            vmem((nx * nz, size // (nx * nz), per_z), BF16),
            sems(1 + 2 * STEPS),
            sems(16),
            sems(2),
            sems(nx - 1),
            sems(1),
            sems(1),
            sems(nc // 2 - 1),
            sems(1),
            sems(1),
            sems(nx - 1),
            sems(nx - 1),
            sems(1),
            sems(nc // 2 - 1),
            sems(1),
            sems(2),
            sems(1),
        ],
        compiler_params=pltpu.CompilerParams(
            collective_id=0, has_side_effects=True, vmem_limit_bytes=VMEM_LIMIT
        ),
    )(row_features.T, col_features.T, test_block)
    basis_t, projected = pl.pallas_call(
        finish,
        out_shape=(
            jax.ShapeDtypeStruct((share, rows), F32),
            jax.ShapeDtypeStruct((size // (nx * nz), columns), F32),
        ),
        in_specs=[pl.BlockSpec(memory_space=vmem)] * 2,
        out_specs=(pl.BlockSpec(memory_space=pl.ANY),) * 2,
        scratch_shapes=[vmem((size // (nx * nz), columns), F32), sems(2)],
        compiler_params=pltpu.CompilerParams(vmem_limit_bytes=2 * 1024 * 1024),
    )(basis_t, pieces)
    return basis_t.T, projected


def solution(mesh, nx=ALONG_X):
    nz, nc = mesh.shape["rows"] // nx, mesh.shape["cols"]
    return jax.shard_map(
        functools.partial(local, nx, nz, nc),
        mesh=mesh,
        in_specs=(P("rows", None), P("cols", None), P("cols", None)),
        out_specs=(P("rows", "cols"), P("rows", "cols")),
        check_vma=False,
    )
```
